32 devices in a mesh: dp: 2 (over y), expert: 4 (over z), ffn: 4 (over x, core).
Axes of the slice: x: 2, y: 2, z: 4, core: 2. Of those that a mesh axis runs over, the one named last changes fastest.
Arguments:
- tokens: bfloat16 [512, 4096], P('expert'), may hold values from -6 to 6
- expert_ids: int32 [512, 2], P('expert'), may hold values from 0 to 3, all different within a row; in each aligned block of 128 rows (0 to 127, 128 to 255, ...) at most 64 rows name the same one
- route_weight: float32 [512, 2], P('expert'), may hold values from 0.05 to 1
- cotangent: bfloat16 [512, 4096], P('expert'), may hold values from -40 to 40
- w_gate: bfloat16 [4, 7168, 4096], P('expert', ('dp', 'ffn')), may hold values from -0.09375 to 0.09375
- w_up: bfloat16 [4, 7168, 4096], P('expert', ('dp', 'ffn')), may hold values from -0.09375 to 0.09375
- w_down: bfloat16 [4, 7168, 4096], P('expert', ('dp', 'ffn')), may hold values from -0.0625 to 0.0625
Outputs:
- layer_out: bfloat16 [512, 4096], P('expert', ('dp', 'ffn'))
- ascent_gate: bfloat16 [4, 7168, 4096], P('expert', ('dp', 'ffn'))
- ascent_up: bfloat16 [4, 7168, 4096], P('expert', ('dp', 'ffn'))
- ascent_down: bfloat16 [4, 7168, 4096], P('expert', ('dp', 'ffn'))
The draws below stay inside these ranges and needn't reach their ends.
Inputs may be any that keep to these rules, and one draw needn't show every extreme that they name: `expert_ids`: each row names two different experts. Among the rows of one aligned block of 128 no expert is named more than 64 times; in every draw some block names some expert exactly 64 times.
All inputs are finite; a program needn't handle non-finite values.
Results may differ from the reference program's by a relative error of at most 0.017.
Values may be sent and summed in bfloat16 or wider, within the bound.
A program may use at most 128 MiB of HBM per device.

```python
import math
import jax
import jax.numpy as jnp
import numpy as np
from jax import lax

D = 4096
FF = 7168
TOP = 2
TOK_DEV = 128
EXPERTS = 4
CAP = 64
TOKENS = 512
SLOTS = 256
GROUPS = 8


def draw_cotangent(key, part):
    base_key, row_key, col_key = jax.random.split(key, 3)
    row_count = TOKENS
    position = jnp.arange(row_count, dtype=jnp.float32) / row_count
    row_scale = jnp.exp(jax.random.uniform(row_key, (row_count, 1), jnp.float32, 0.0, 2.3))
    col_scale = jnp.exp(jax.random.uniform(col_key, (1, D), jnp.float32, 0.0, 1.1))
    values = jnp.clip(jax.random.normal(base_key, (row_count, D), jnp.float32), -4.0, 4.0) * (3.0 ** position)[:, None]
    return jnp.clip(values * row_scale * col_scale * 0.3, -40.0, 40.0).astype(jnp.bfloat16)


def shard_levels(own_key, shape, cuts, least, high):
    factor_of = 1.0
    for axis_at, shards_of in cuts:
        heights = jax.random.uniform(jax.random.fold_in(jax.random.fold_in(own_key, 6), axis_at), (shards_of,), jnp.float32, least / len(cuts), high / len(cuts))
        factor_of = factor_of * jnp.repeat(jnp.exp(heights), shape[axis_at] // shards_of).reshape((-1,) + (1,) * (len(shape) - 1 - axis_at))
    return factor_of


def deal_out(stream_key, own, number, rows, amount, top, bound, slope):
    ranking = jax.random.permutation(stream_key, amount)
    crowded, ordinary = shares(amount, rows * top, bound, slope, True), shares(amount, rows * top, bound, slope, False)
    places = jnp.arange(amount)

    def named(sizes, rotation):
        used = int((sizes > 0).sum())
        fixed = max(1, used // 4)
        shifted = fixed + (places - fixed + rotation * (used - fixed)) % max(1, amount - fixed)
        return jnp.zeros((amount,), jnp.int32).at[ranking[jnp.where(places < fixed, places, shifted)]].set(jnp.asarray(sizes, jnp.int32))

    sizes = jnp.where(number % 4 == 0, named(crowded, number // 4), named(ordinary, number - number // 4 - 1))
    mixed = jax.random.permutation(jax.random.fold_in(own, 3), amount)
    source_of, taker = mixed[0:amount // 2 * 2:2], mixed[1:amount // 2 * 2:2]
    slack = jnp.minimum(sizes[source_of] - 1, bound - sizes[taker]) // 2
    slack = jnp.where((source_of == ranking[0]) | (taker == ranking[0]) | (sizes[taker] == 0), 0, jnp.maximum(slack, 0))
    shifted = jax.random.randint(jax.random.fold_in(own, 4), (amount // 2,), 0, 1 << 20) % (slack + 1)
    sizes = sizes.at[source_of].add(-shifted).at[taker].add(shifted)
    members = jnp.searchsorted(jnp.cumsum(sizes), jnp.arange(rows * top), side="right").astype(jnp.int32)
    grid = members.reshape(top, rows).T
    grid = grid[jax.random.permutation(jax.random.fold_in(own, 1), rows)]
    rotation = jax.random.randint(jax.random.fold_in(own, 2), (rows, 1), 0, top)
    return jnp.take_along_axis(grid, (jnp.arange(top)[None, :] + rotation) % top, axis=1)


def shares(number_of, total, limit, lean, full):
    weights = [(1 << 20) // math.isqrt(grade ** lean) + 1 for grade in range(1, number_of + 1)]
    largest = limit if full else min(limit, max(-(-total // number_of), total * weights[0] // sum(weights)))
    least = 1 if total - largest >= number_of - 1 else 0
    counts, spare = [largest] + [least] * (number_of - 1), total - largest - least * (number_of - 1)
    while spare > 0:
        movable = [i for i in range(1, number_of) if counts[i] < largest] or [i for i in range(1, number_of) if counts[i] < limit]
        mass, budget = sum([weights[i] for i in movable]), spare
        for i in movable:
            more = min(limit - counts[i], max(1, budget * weights[i] // mass), spare)
            counts[i] = counts[i] + more
            spare = spare - more
    return np.array(counts)


def bell_draw(own_key, extent, width, most, cuts=(), held_as=jnp.bfloat16):
    entries = jax.random.normal(own_key, extent, jnp.float32) * width
    if len(cuts) > 0:
        entries = shard_levels(own_key, extent, cuts, -0.22, 0.18) * entries
    return jnp.clip(entries, min=-most, max=most).astype(held_as)


def setup_inputs(seed: int = 0) -> dict:
    key_of = jax.random.split(jax.random.key(seed), 8)
    tokens = bell_draw(key_of[0], (TOKENS, D), 1.0, 6.0, ((0, 4),))
    expert_ids_keys = jax.random.split(jax.random.fold_in(key_of[1], 1), TOKENS // TOK_DEV)
    expert_ids_turns = jax.random.permutation(jax.random.fold_in(key_of[1], 3), TOKENS // TOK_DEV)
    expert_ids = jax.vmap(lambda own, number: deal_out(jax.random.fold_in(key_of[1], 2), own, number, TOK_DEV, EXPERTS, TOP, CAP, 2))(expert_ids_keys, expert_ids_turns).reshape((TOKENS, TOP))
    route_weight = jnp.clip(0.05 + 0.95 * jax.random.uniform(key_of[2], (TOKENS, TOP), jnp.float32) ** shard_levels(key_of[2], (TOKENS, TOP), ((0, 4),), -0.2, 0.2), 0.05, 1.0)
    cotangent = draw_cotangent(jax.random.fold_in(key_of[7], 71), 0)
    w_gate = bell_draw(key_of[4], (EXPERTS, FF, D), D ** -0.5, 0.09375, ((0, 4), (1, 8)))
    w_up = bell_draw(key_of[5], (EXPERTS, FF, D), D ** -0.5, 0.09375, ((0, 4), (1, 8)))
    w_down = bell_draw(key_of[6], (EXPERTS, FF, D), FF ** -0.5, 0.0625, ((0, 4), (1, 8)))
    return {"tokens": tokens, "expert_ids": expert_ids, "route_weight": route_weight, "cotangent": cotangent, "w_gate": w_gate, "w_up": w_up, "w_down": w_down}


def silu_parts(pre_act):
    sigmoid_value = jax.nn.sigmoid(pre_act)
    return (pre_act * sigmoid_value, sigmoid_value * (1.0 + pre_act * (1.0 - sigmoid_value)))

def against_rows(left_rows, right_rows):
    return lax.dot_general(left_rows.astype(jnp.float32), right_rows.astype(jnp.float32), (((0,), (0,)), ((), ())))

def across_width(left_rows, weight):
    return lax.dot_general(left_rows.astype(jnp.float32), weight.astype(jnp.float32), (((1,), (1,)), ((), ())))

def reference(tokens, expert_ids, route_weight, cotangent, w_gate, w_up, w_down):
    block_count = TOKENS // TOK_DEV
    route_ids = expert_ids.reshape(block_count, TOK_DEV, 2)
    chosen = route_ids[:, :, :, None] == jnp.arange(EXPERTS, dtype=jnp.int32)
    per_token = lax.optimization_barrier(jnp.sum(chosen.astype(jnp.int32), axis=2)).astype(jnp.int32)
    earlier = (jnp.cumsum(per_token, axis=1) - per_token).astype(jnp.int32)
    position = lax.optimization_barrier(jnp.sum(jnp.where(chosen, earlier[:, :, None, :], 0), axis=3)).astype(jnp.int32)
    block_start = (jnp.arange(block_count, dtype=jnp.int32) * CAP)[:, None, None]
    flat_slot = (route_ids * SLOTS + block_start + position).reshape(-1).astype(jnp.int32)
    scaled = (route_weight[:, :, None] * cotangent.astype(jnp.float32)[:, None, :]).astype(jnp.bfloat16)
    token_table = jnp.zeros((EXPERTS * SLOTS, D), jnp.bfloat16).at[flat_slot].set(jnp.repeat(tokens, 2, axis=0))
    grad_table = jnp.zeros((EXPERTS * SLOTS, D), jnp.bfloat16).at[flat_slot].set(scaled.reshape(TOKENS * 2, D))
    group_width = FF // GROUPS

    def one_expert(operands):
        slot_rows, slot_grads, gate_weight, up_weight, down_weight = operands
        pre_gate = across_width(slot_rows, gate_weight)
        pre_up = across_width(slot_rows, up_weight)
        activated, derivative = silu_parts(pre_gate)
        hidden = (activated * pre_up).astype(jnp.bfloat16)

        def add_group(running, part_index):
            start = (part_index * group_width).astype(jnp.int32)
            hidden_part = lax.dynamic_slice_in_dim(hidden, start, group_width, 1)
            weight_part = lax.dynamic_slice_in_dim(down_weight, start, group_width, 0)
            product = jnp.dot(hidden_part.astype(jnp.float32), weight_part.astype(jnp.float32))
            rounded = lax.optimization_barrier(product.astype(jnp.bfloat16))
            return (running + rounded.astype(jnp.float32), None)
        summed, _ = lax.scan(add_group, jnp.zeros((SLOTS, D), jnp.float32), jnp.arange(GROUPS, dtype=jnp.int32))
        grad_down = against_rows(hidden, slot_grads)
        grad_hidden = across_width(slot_grads, down_weight)
        delta_gate = (grad_hidden * pre_up * derivative).astype(jnp.bfloat16)
        delta_up = (grad_hidden * activated).astype(jnp.bfloat16)
        return (summed.astype(jnp.bfloat16), against_rows(delta_gate, slot_rows), against_rows(delta_up, slot_rows), grad_down)
    slot_out, grads_gate, grads_up, grads_down = lax.map(one_expert, (token_table.reshape(EXPERTS, SLOTS, D), grad_table.reshape(EXPERTS, SLOTS, D), w_gate, w_up, w_down))
    picked = slot_out.reshape(EXPERTS * SLOTS, D)[flat_slot].astype(jnp.float32).reshape(TOKENS, 2, D)
    layer_out = lax.optimization_barrier(jnp.sum(route_weight[:, :, None] * picked, axis=1)).astype(jnp.bfloat16)
    sum_squares = jnp.sum(grads_gate * grads_gate) + jnp.sum(grads_up * grads_up) + jnp.sum(grads_down * grads_down)
    inv_rms = lax.rsqrt(sum_squares / (3.0 * EXPERTS * FF * D) + 1e-06)
    return (layer_out, (grads_gate * inv_rms).astype(jnp.bfloat16), (grads_up * inv_rms).astype(jnp.bfloat16), (grads_down * inv_rms).astype(jnp.bfloat16))
```

```python
import functools

import jax
import jax.numpy as jnp
from jax import lax
from jax.experimental import pallas as pl
from jax.experimental.pallas import tpu as pltpu
from jax.sharding import PartitionSpec as P

CORES = 2


def silu_parts(pre_act):
    sigmoid_value = jax.nn.sigmoid(pre_act)
    return (pre_act * sigmoid_value, sigmoid_value * (1.0 + pre_act * (1.0 - sigmoid_value)))


def against_rows(left_rows, right_rows):
    return lax.dot_general(
        left_rows, right_rows, (((0,), (0,)), ((), ())), preferred_element_type=jnp.float32
    )


def across_width(left_rows, weight):
    return lax.dot_general(
        left_rows, weight, (((1,), (1,)), ((), ())), preferred_element_type=jnp.float32
    )


def remote(src, dst, send_sem, recv_sem, device):
    return pltpu.make_async_remote_copy(
        src_ref=src,
        dst_ref=dst,
        send_sem=send_sem,
        recv_sem=recv_sem,
        device_id=device,
        device_id_type=pl.DeviceIdType.MESH,
    )


class Place:
    def __init__(self, ny, nz, nx, width):
        self.ny, self.nz, self.nx, self.width = ny, nz, nx, width
        self.y = lax.axis_index("dp")
        self.z = lax.axis_index("expert")
        ffn = lax.axis_index("ffn")
        self.x, self.c = ffn // CORES, lax.rem(ffn, CORES)

    def at(self, dy=0, dz=0, dx=0, other=False):
        core = 1 - self.c if other else self.c
        return (
            lax.rem(self.y + dy + self.ny, self.ny),
            lax.rem(self.z + dz + self.nz, self.nz),
            lax.rem(self.x + dx + self.nx, self.nx) * CORES + core,
        )

    def cols(self, dy=0, dx=0, other=False):
        y, _, ffn = self.at(dy, 0, dx, other)
        group = y * (self.nx * CORES) + ffn
        return pl.ds(pl.multiple_of(group * self.width, self.width), self.width)

    def greet(self):
        peers = [self.at(other=True)]
        peers += [self.at(dx=i) for i in range(1, self.nx)]
        peers += [self.at(dy=k) for k in range(1, self.ny)]
        peers += [self.at(dz=j) for j in range(1, self.nz)]
        return peers

    def enter(self, more=()):
        barrier = pltpu.get_barrier_semaphore()
        peers = self.greet() + list(more)
        for peer in peers:
            pl.semaphore_signal(
                barrier, inc=1, device_id=peer, device_id_type=pl.DeviceIdType.MESH
            )
        pl.semaphore_wait(barrier, len(peers))


def dispatch_kernel(
    ny, nz, nx, cap, width, tok, grad, rows, grads,
    own_sem, zs, zr, xs, xr, ys, yr, us, ur, ls, lr, ds, dr,
):
    here = Place(ny, nz, nx, width)
    here.enter()
    source, target = (tok, grad), (rows, grads)
    pending = []

    def block(dz):
        return pl.multiple_of(here.at(dz=dz)[1] * cap, cap)

    for a in range(2):
        for j in range(1, nz):
            unit = a * (nz - 1) + j - 1
            copy = remote(
                source[a].at[pl.ds(block(j), cap), here.cols()],
                target[a].at[pl.ds(block(0), cap), here.cols()],
                zs.at[unit], zr.at[unit], here.at(dz=j),
            )
            copy.start()
            pending.append(copy)
    local = []
    for a in range(2):
        copy = pltpu.make_async_copy(
            source[a].at[pl.ds(block(0), cap), :],
            target[a].at[pl.ds(block(0), cap), :],
            own_sem.at[a],
        )
        copy.start()
        local.append(copy)

    def piece(unit, dy=0, dx=0, other=False, half=None):
        a, j = unit // (nz - 1), unit % (nz - 1) + 1
        first, count = block(-j), cap
        if half is not None:
            count = cap // 2
            first = pl.multiple_of(first + half * count, count)
        return target[a].at[pl.ds(first, count), here.cols(dy, dx, other)]

    def push(ref, send_sem, recv_sem, device):
        copy = remote(ref, ref, send_sem, recv_sem, device)
        copy.start()
        pending.append(copy)

    def arrived(ref, send_sem, recv_sem):
        remote(ref, ref, send_sem, recv_sem, here.at(other=True)).wait_recv()

    def first(u):
        arrived(piece(u), zs.at[u], zr.at[u])
        for i in range(1, nx):
            push(piece(u), xs.at[u, i - 1], xr.at[u, i - 1], here.at(dx=i))
        for k in range(1, ny):
            push(piece(u), ys.at[u, k - 1], yr.at[u, k - 1], here.at(dy=k))
        push(piece(u), ds.at[u, 0], dr.at[u, 0], here.at(other=True))

    def second(u):
        for i in range(1, nx):
            arrived(piece(u, dx=-i), xs.at[u, i - 1], xr.at[u, i - 1])
            for k in range(1, ny):
                at = (i - 1) * (ny - 1) + k - 1
                push(piece(u, dx=-i, half=0), us.at[u, at], ur.at[u, at], here.at(dy=k))
            push(piece(u, dx=-i), ds.at[u, i], dr.at[u, i], here.at(other=True))
        for k in range(1, ny):
            arrived(piece(u, dy=-k), ys.at[u, k - 1], yr.at[u, k - 1])
            for i in range(1, nx):
                at = (i - 1) * (ny - 1) + k - 1
                push(piece(u, dy=-k, half=1), ls.at[u, at], lr.at[u, at], here.at(dx=i))
            push(piece(u, dy=-k), ds.at[u, k * nx], dr.at[u, k * nx], here.at(other=True))

    def third(u):
        for i in range(1, nx):
            for k in range(1, ny):
                at = (i - 1) * (ny - 1) + k - 1
                arrived(piece(u, -k, -i, half=0), us.at[u, at], ur.at[u, at])
                arrived(piece(u, -k, -i, half=1), ls.at[u, at], lr.at[u, at])
                to = k * nx + i
                push(piece(u, -k, -i), ds.at[u, to], dr.at[u, to], here.at(other=True))

    def fourth(u):
        for i in range(nx):
            for k in range(ny):
                to = k * nx + i
                arrived(piece(u, -k, -i, True), ds.at[u, to], dr.at[u, to])

    units = 2 * (nz - 1)
    stages = (first, second, third, fourth)
    for step in range(units + len(stages) - 1):
        for late, stage in enumerate(stages):
            if 0 <= step - late < units:
                stage(step - late)
    for copy in local:
        copy.wait()
    for copy in pending:
        copy.wait_send()


def dispatch(sizes, tok, grad):
    ny, nz, nx, cap, width = sizes
    units, chips = 2 * (nz - 1), nx * ny
    diag = max(1, (nx - 1) * (ny - 1))
    dma = pltpu.SemaphoreType.DMA
    pair = lambda *shape: [dma(shape), dma(shape)]
    vmem = pl.BlockSpec(memory_space=pltpu.VMEM)
    return pl.pallas_call(
        functools.partial(dispatch_kernel, *sizes),
        out_shape=[jax.ShapeDtypeStruct(tok.shape, tok.dtype)] * 2,
        in_specs=[vmem] * 2,
        out_specs=[vmem] * 2,
        scratch_shapes=[
            dma((2,)),
            *pair(units), *pair(units, max(1, nx - 1)), *pair(units, max(1, ny - 1)),
            *pair(units, diag), *pair(units, diag), *pair(units, chips),
        ],
        compiler_params=pltpu.CompilerParams(collective_id=0, has_side_effects=True),
    )(tok, grad)


def combine_kernel(
    ny, nz, nx, cap, width, part, sq, ret, sq_out,
    pair, out_buf, in_buf, acc, summed, sq_own, sq_in,
    ps, pr, cs, cr, zs, zr, ss, sr,
):
    here = Place(ny, nz, nx, width)
    for_diag = [(k, i) for k in range(1, ny) for i in range(1, nx)]
    here.enter([here.at(k, 0, i) for k, i in for_diag])
    order = for_diag + [(0, i) for i in range(1, nx)] + [(k, 0) for k in range(1, ny)] + [(0, 0)]
    pending = []

    def started(copy):
        copy.start()
        pending.append(copy)
        return copy

    partner = here.at(other=True)
    swaps = {}
    for k, i in order:
        o = k * nx + i
        swaps[o] = started(
            remote(part.at[:, here.cols(k, i, True)], pair.at[o], ps.at[o], pr.at[o], partner)
        )

    def stage(level, peers, base):
        for n, (to, _) in enumerate(peers):
            started(
                remote(sq_own.at[level], sq_in.at[base + n], ss.at[base + n], sr.at[base + n], to)
            )
        total = sq_own[level]
        for n in range(len(peers)):
            remote(
                sq_own.at[level], sq_in.at[base + n], ss.at[base + n], sr.at[base + n], partner
            ).wait_recv()
            total = total + sq_in[base + n]
        sq_own[level + 1] = total
        return base + len(peers)

    sq_own[0] = sq[...]
    base = stage(0, [(partner, 0)], 0)
    for k, i in order:
        o = k * nx + i
        swaps[o].wait_recv()
        total = part[:, here.cols(k, i)].astype(jnp.float32) + pair[o].astype(jnp.float32)
        if o == 0:
            acc[...] = total
        else:
            out_buf[o] = total.astype(jnp.bfloat16)
            started(
                remote(out_buf.at[o], in_buf.at[o], cs.at[o], cr.at[o], here.at(k, 0, i))
            )
    base = stage(1, [(here.at(dz=j), 0) for j in range(1, nz)], base)
    base = stage(2, [(here.at(dx=i), 0) for i in range(1, nx)], base)
    base = stage(3, [(here.at(dy=k), 0) for k in range(1, ny)], base)
    sq_out[...] = sq_own[4]
    for o in range(1, nx * ny):
        remote(out_buf.at[o], in_buf.at[o], cs.at[o], cr.at[o], partner).wait_recv()
    total = acc[...]
    for o in range(1, nx * ny):
        total = total + in_buf[o].astype(jnp.float32)
    summed[...] = total.astype(jnp.bfloat16)

    def block(dz):
        return pl.ds(pl.multiple_of(here.at(dz=dz)[1] * cap, cap), cap)

    backs = []
    for j in range(1, nz):
        backs.append(
            started(
                remote(
                    summed.at[block(j), :], ret.at[block(0), :],
                    zs.at[j - 1], zr.at[j - 1], here.at(dz=j),
                )
            )
        )
    ret[block(0), :] = summed[block(0), :]
    for copy in backs:
        copy.wait_recv()
    for copy in pending:
        copy.wait_send()


def combine(sizes, part, square):
    ny, nz, nx, cap, width = sizes
    slots, chips = nz * cap, nx * ny
    peers = 1 + (nz - 1) + (nx - 1) + (ny - 1)
    dma = pltpu.SemaphoreType.DMA
    twice = lambda count: [dma((count,)), dma((count,))]
    vmem = pl.BlockSpec(memory_space=pltpu.VMEM)
    flat = jnp.full((8, 128), square, jnp.float32)
    return pl.pallas_call(
        functools.partial(combine_kernel, *sizes),
        out_shape=[
            jax.ShapeDtypeStruct((slots, width), jnp.bfloat16),
            jax.ShapeDtypeStruct((8, 128), jnp.float32),
        ],
        in_specs=[vmem] * 2,
        out_specs=[vmem] * 2,
        scratch_shapes=[
            *[pltpu.VMEM((chips, slots, width), jnp.bfloat16)] * 3,
            pltpu.VMEM((slots, width), jnp.float32),
            pltpu.VMEM((slots, width), jnp.bfloat16),
            pltpu.VMEM((5, 8, 128), jnp.float32),
            pltpu.VMEM((peers, 8, 128), jnp.float32),
            *twice(chips), *twice(chips), *twice(max(1, nz - 1)), *twice(peers),
        ],
        compiler_params=pltpu.CompilerParams(
            collective_id=1, has_side_effects=True, vmem_limit_bytes=48 * 1024 * 1024
        ),
    )(part, flat)


def on_device(sizes, count, tokens, expert_ids, route_weight, cotangent, w_gate, w_up, w_down):
    ny, experts, nx, capacity, column_width = sizes
    tok_rows, feature_width = tokens.shape
    slot_count = experts * capacity
    chosen = expert_ids[:, :, None] == jnp.arange(experts, dtype=jnp.int32)[None, None, :]
    per_token = jnp.sum(chosen.astype(jnp.bfloat16), axis=1)
    row = jnp.arange(tok_rows, dtype=jnp.int32)
    before = (row[None, :] < row[:, None]).astype(jnp.bfloat16)
    earlier = jnp.dot(before, per_token, preferred_element_type=jnp.float32).astype(jnp.int32)
    position = jnp.sum(jnp.where(chosen, earlier[:, None, :], 0), axis=2)
    slot_index = expert_ids * capacity + position
    slots = jnp.arange(slot_count, dtype=jnp.int32)
    hot = [slot_index[:, k][None, :] == slots[:, None] for k in range(2)]
    hot_any = (hot[0] | hot[1]).astype(jnp.bfloat16)
    token_slots = jnp.dot(hot_any, tokens, preferred_element_type=jnp.float32).astype(jnp.bfloat16)
    picked_cot = jnp.dot(hot_any, cotangent, preferred_element_type=jnp.float32)
    slot_weight = jnp.sum(
        jnp.where(hot[0], route_weight[:, 0][None, :], 0.0)
        + jnp.where(hot[1], route_weight[:, 1][None, :], 0.0),
        axis=1,
    )
    grad_slots = (slot_weight[:, None] * picked_cot).astype(jnp.bfloat16)
    slot_rows, slot_grads = dispatch(sizes, token_slots, grad_slots)
    gate_weight, up_weight, down_weight = w_gate[0], w_up[0], w_down[0]
    pre_gate = across_width(slot_rows, gate_weight)
    pre_up = across_width(slot_rows, up_weight)
    activated, derivative = silu_parts(pre_gate)
    hidden = (activated * pre_up).astype(jnp.bfloat16)
    partial_value = jnp.dot(hidden, down_weight, preferred_element_type=jnp.float32)
    grad_hidden = across_width(slot_grads, down_weight)
    delta_gate = (grad_hidden * pre_up * derivative).astype(jnp.bfloat16)
    delta_up = (grad_hidden * activated).astype(jnp.bfloat16)
    gram_rows = across_width(slot_rows, slot_rows)
    gram_grads = across_width(slot_grads, slot_grads)
    gram_delta = across_width(delta_gate, delta_gate) + across_width(delta_up, delta_up)
    square = jnp.sum(gram_rows * gram_delta) + jnp.sum(gram_grads * across_width(hidden, hidden))
    returned_rows, square_all = combine(sizes, partial_value.astype(jnp.bfloat16), square)
    weight_hot = [h.astype(jnp.bfloat16) for h in hot]
    picked = [against_rows(h, returned_rows) for h in weight_hot]
    layer_out = (route_weight[:, 0:1] * picked[0] + route_weight[:, 1:2] * picked[1]).astype(
        jnp.bfloat16
    )
    inv_rms = lax.rsqrt(jnp.maximum(square_all[0, 0], 0.0) / count + 1e-06)
    return (
        layer_out,
        (against_rows(delta_gate, slot_rows) * inv_rms).astype(jnp.bfloat16)[None],
        (against_rows(delta_up, slot_rows) * inv_rms).astype(jnp.bfloat16)[None],
        (against_rows(hidden, slot_grads) * inv_rms).astype(jnp.bfloat16)[None],
    )


def solution(mesh):
    ny, nz, nx = mesh.shape["dp"], mesh.shape["expert"], mesh.shape["ffn"] // CORES

    def body(*args):
        tok_rows, feature_width = args[0].shape
        sizes = (ny, nz, nx, tok_rows // 2, feature_width // (ny * nx * CORES))
        count = 3.0 * nz * args[4].shape[1] * (ny * nx * CORES) * feature_width
        return on_device(sizes, count, *args)

    return jax.shard_map(
        body,
        mesh=mesh,
        in_specs=(
            P("expert", None),
            P("expert", None),
            P("expert", None),
            P("expert", None),
            P("expert", ("dp", "ffn"), None),
            P("expert", ("dp", "ffn"), None),
            P("expert", ("dp", "ffn"), None),
        ),
        out_specs=(
            P("expert", ("dp", "ffn")),
            P("expert", ("dp", "ffn"), None),
            P("expert", ("dp", "ffn"), None),
            P("expert", ("dp", "ffn"), None),
        ),
        check_vma=False,
    )
```

```python
import functools

import jax
import jax.numpy as jnp
from jax import lax
from jax.experimental import pallas as pl
from jax.experimental.pallas import tpu as pltpu
from jax.sharding import PartitionSpec as P

CORES = 2


def silu_parts(pre_act):
    sigmoid_value = jax.nn.sigmoid(pre_act)
    return (pre_act * sigmoid_value, sigmoid_value * (1.0 + pre_act * (1.0 - sigmoid_value)))


def against_rows(left_rows, right_rows):
    return lax.dot_general(
        left_rows, right_rows, (((0,), (0,)), ((), ())), preferred_element_type=jnp.float32
    )


def across_width(left_rows, weight):
    return lax.dot_general(
        left_rows, weight, (((1,), (1,)), ((), ())), preferred_element_type=jnp.float32
    )


def along(left, right):
    return jnp.dot(left, right, preferred_element_type=jnp.float32)


def remote(src, dst, send_sem, recv_sem, device):
    return pltpu.make_async_remote_copy(
        src_ref=src,
        dst_ref=dst,
        send_sem=send_sem,
        recv_sem=recv_sem,
        device_id=device,
        device_id_type=pl.DeviceIdType.MESH,
    )


class Place:
    def __init__(self, ny, nz, nx, width):
        self.ny, self.nz, self.nx, self.width = ny, nz, nx, width
        self.y = lax.axis_index("dp")
        self.z = lax.axis_index("expert")
        ffn = lax.axis_index("ffn")
        self.x, self.c = ffn // CORES, lax.rem(ffn, CORES)

    def at(self, dy=0, dz=0, dx=0, other=False):
        core = 1 - self.c if other else self.c
        return (
            lax.rem(self.y + dy + self.ny, self.ny),
            lax.rem(self.z + dz + self.nz, self.nz),
            lax.rem(self.x + dx + self.nx, self.nx) * CORES + core,
        )

    def cols(self, dy=0, dx=0, other=False):
        y, _, ffn = self.at(dy, 0, dx, other)
        group = y * (self.nx * CORES) + ffn
        return pl.ds(pl.multiple_of(group * self.width, self.width), self.width)

    def greet(self):
        peers = [self.at(other=True)]
        peers += [self.at(dx=i) for i in range(1, self.nx)]
        peers += [self.at(dy=k) for k in range(1, self.ny)]
        peers += [self.at(dz=j) for j in range(1, self.nz)]
        return peers

    def enter(self, more=()):
        barrier = pltpu.get_barrier_semaphore()
        peers = self.greet() + list(more)
        for peer in peers:
            pl.semaphore_signal(
                barrier, inc=1, device_id=peer, device_id_type=pl.DeviceIdType.MESH
            )
        pl.semaphore_wait(barrier, len(peers))


def against_slots(weight, slots, out):
    tile = weight.shape[0] // 2

    def half(n, carry):
        at = pl.ds(pl.multiple_of(n * tile, tile), tile)
        out[at, :] = across_width(weight[at, :], slots[...])
        return carry

    lax.fori_loop(0, 2, half, 0)


def dispatch_kernel(
    ny, nz, nx, cap, width, tok, grad, wg, wu, wd, rows, grads, gate_t, up_t, hid_t, part,
    wg_v, wu_v, wd_v, w_sem, own_sem, zs, zr, xs, xr, ys, yr, us, ur, ls, lr, ds, dr,
):
    here = Place(ny, nz, nx, width)
    loads = []
    for n, (weight, held) in enumerate(((wg, wg_v), (wu, wu_v), (wd, wd_v))):
        loads.append(pltpu.make_async_copy(weight, held, w_sem.at[n]))
        loads[-1].start()
    here.enter()
    source, target = (tok, grad), (rows, grads)
    pending = []

    def block(dz):
        return pl.multiple_of(here.at(dz=dz)[1] * cap, cap)

    for a in range(2):
        for j in range(1, nz):
            unit = a * (nz - 1) + j - 1
            copy = remote(
                source[a].at[pl.ds(block(j), cap), here.cols()],
                target[a].at[pl.ds(block(0), cap), here.cols()],
                zs.at[unit], zr.at[unit], here.at(dz=j),
            )
            copy.start()
            pending.append(copy)
    local = []
    for a in range(2):
        copy = pltpu.make_async_copy(
            source[a].at[pl.ds(block(0), cap), :],
            target[a].at[pl.ds(block(0), cap), :],
            own_sem.at[a],
        )
        copy.start()
        local.append(copy)

    def piece(unit, dy=0, dx=0, other=False, half=None):
        a, j = unit // (nz - 1), unit % (nz - 1) + 1
        first, count = block(-j), cap
        if half is not None:
            count = cap // 2
            first = pl.multiple_of(first + half * count, count)
        return target[a].at[pl.ds(first, count), here.cols(dy, dx, other)]

    def push(ref, send_sem, recv_sem, device):
        copy = remote(ref, ref, send_sem, recv_sem, device)
        copy.start()
        pending.append(copy)

    def arrived(ref, send_sem, recv_sem):
        remote(ref, ref, send_sem, recv_sem, here.at(other=True)).wait_recv()

    def first(u):
        arrived(piece(u), zs.at[u], zr.at[u])
        for i in range(1, nx):
            push(piece(u), xs.at[u, i - 1], xr.at[u, i - 1], here.at(dx=i))
        for k in range(1, ny):
            push(piece(u), ys.at[u, k - 1], yr.at[u, k - 1], here.at(dy=k))
        push(piece(u), ds.at[u, 0], dr.at[u, 0], here.at(other=True))

    def second(u):
        for i in range(1, nx):
            arrived(piece(u, dx=-i), xs.at[u, i - 1], xr.at[u, i - 1])
            for k in range(1, ny):
                at = (i - 1) * (ny - 1) + k - 1
                push(piece(u, dx=-i, half=0), us.at[u, at], ur.at[u, at], here.at(dy=k))
            push(piece(u, dx=-i), ds.at[u, i], dr.at[u, i], here.at(other=True))
        for k in range(1, ny):
            arrived(piece(u, dy=-k), ys.at[u, k - 1], yr.at[u, k - 1])
            for i in range(1, nx):
                at = (i - 1) * (ny - 1) + k - 1
                push(piece(u, dy=-k, half=1), ls.at[u, at], lr.at[u, at], here.at(dx=i))
            push(piece(u, dy=-k), ds.at[u, k * nx], dr.at[u, k * nx], here.at(other=True))

    def third(u):
        for i in range(1, nx):
            for k in range(1, ny):
                at = (i - 1) * (ny - 1) + k - 1
                arrived(piece(u, -k, -i, half=0), us.at[u, at], ur.at[u, at])
                arrived(piece(u, -k, -i, half=1), ls.at[u, at], lr.at[u, at])
                to = k * nx + i
                push(piece(u, -k, -i), ds.at[u, to], dr.at[u, to], here.at(other=True))

    def fourth(u):
        for i in range(nx):
            for k in range(ny):
                to = k * nx + i
                arrived(piece(u, -k, -i, True), ds.at[u, to], dr.at[u, to])

    def gate():
        local[0].wait()
        loads[0].wait()
        against_slots(wg_v, rows, gate_t)

    def up():
        loads[1].wait()
        against_slots(wu_v, rows, up_t)
        activated, _ = silu_parts(gate_t[...])
        hid_t[...] = (activated * up_t[...]).astype(jnp.bfloat16)

    def down():
        loads[2].wait()
        tile = rows.shape[1] // 8

        def columns(n, carry):
            at = pl.ds(pl.multiple_of(n * tile, tile), tile)
            part[:, at] = against_rows(hid_t[...], wd_v[:, at]).astype(jnp.bfloat16)
            return carry

        lax.fori_loop(0, 8, columns, 0)

    work = [gate, up, down]
    units = 2 * (nz - 1)
    stages = (first, second, third, fourth)
    for step in range(units + len(stages) - 1):
        for late, stage in enumerate(stages):
            if 0 <= step - late < units:
                stage(step - late)
        if step >= nz + 1 and work:
            work.pop(0)()
    for task in work:
        task()
    local[1].wait()
    for copy in pending:
        copy.wait_send()


def dispatch(sizes, tok, grad, wg, wu, wd):
    ny, nz, nx, cap, width = sizes
    units, chips = 2 * (nz - 1), nx * ny
    diag = max(1, (nx - 1) * (ny - 1))
    dma = pltpu.SemaphoreType.DMA
    pair = lambda *shape: [dma(shape), dma(shape)]
    vmem = pl.BlockSpec(memory_space=pltpu.VMEM)
    return pl.pallas_call(
        functools.partial(dispatch_kernel, *sizes),
        out_shape=[
            *[jax.ShapeDtypeStruct(tok.shape, tok.dtype)] * 2,
            *[jax.ShapeDtypeStruct((wg.shape[0], tok.shape[0]), jnp.float32)] * 2,
            jax.ShapeDtypeStruct((wg.shape[0], tok.shape[0]), jnp.bfloat16),
            jax.ShapeDtypeStruct(tok.shape, jnp.bfloat16),
        ],
        in_specs=[vmem] * 2 + [pl.BlockSpec(memory_space=pl.ANY)] * 3,
        out_specs=[vmem] * 6,
        scratch_shapes=[
            *[pltpu.VMEM(wg.shape, wg.dtype)] * 3,
            dma((3,)),
            dma((2,)),
            *pair(units), *pair(units, max(1, nx - 1)), *pair(units, max(1, ny - 1)),
            *pair(units, diag), *pair(units, diag), *pair(units, chips),
        ],
        compiler_params=pltpu.CompilerParams(
            collective_id=0, has_side_effects=True, vmem_limit_bytes=56 * 1024 * 1024
        ),
    )(tok, grad, wg, wu, wd)


def combine_kernel(
    ny, nz, nx, cap, width, part, rows, grads, gate_t, up_t, hid_t, wd,
    ret, sq_out, dgate_t, dup_t, gh, wd_v, w_sem, pair, out_buf, in_buf, acc, summed, sq_own, sq_in,
    ps, pr, cs, cr, zs, zr, ss, sr,
):
    here = Place(ny, nz, nx, width)
    for_diag = [(k, i) for k in range(1, ny) for i in range(1, nx)]
    load = pltpu.make_async_copy(wd, wd_v, w_sem)
    load.start()
    here.enter([here.at(k, 0, i) for k, i in for_diag])
    order = for_diag + [(0, i) for i in range(1, nx)] + [(k, 0) for k in range(1, ny)] + [(0, 0)]
    pending = []

    def started(copy):
        copy.start()
        pending.append(copy)
        return copy

    partner = here.at(other=True)
    swaps = {}
    for k, i in order:
        o = k * nx + i
        swaps[o] = started(
            remote(part.at[:, here.cols(k, i, True)], pair.at[o], ps.at[o], pr.at[o], partner)
        )

    def stage(level, peers, base):
        for n, (to, _) in enumerate(peers):
            started(
                remote(sq_own.at[level], sq_in.at[base + n], ss.at[base + n], sr.at[base + n], to)
            )
        total = sq_own[level]
        for n in range(len(peers)):
            remote(
                sq_own.at[level], sq_in.at[base + n], ss.at[base + n], sr.at[base + n], partner
            ).wait_recv()
            total = total + sq_in[base + n]
        sq_own[level + 1] = total
        return base + len(peers)

    for k, i in order:
        o = k * nx + i
        swaps[o].wait_recv()
        total = part[:, here.cols(k, i)].astype(jnp.float32) + pair[o].astype(jnp.float32)
        if o == 0:
            acc[...] = total
        else:
            out_buf[o] = total.astype(jnp.bfloat16)
            started(
                remote(out_buf.at[o], in_buf.at[o], cs.at[o], cr.at[o], here.at(k, 0, i))
            )
    load.wait()
    against_slots(wd_v, grads, gh)
    activated, derivative = silu_parts(gate_t[...])
    dgate_t[...] = (gh[...] * up_t[...] * derivative).astype(jnp.bfloat16)
    dup_t[...] = (gh[...] * activated).astype(jnp.bfloat16)
    delta_gram = against_rows(dgate_t[...], dgate_t[...]) + against_rows(dup_t[...], dup_t[...])
    square = delta_gram * across_width(rows[...], rows[...])
    hidden_gram = against_rows(hid_t[...], hid_t[...])
    square = jnp.sum(square + hidden_gram * across_width(grads[...], grads[...]))
    sq_own[0] = jnp.full((8, 128), square, jnp.float32)
    base = stage(0, [(partner, 0)], 0)
    base = stage(1, [(here.at(dz=j), 0) for j in range(1, nz)], base)
    base = stage(2, [(here.at(dx=i), 0) for i in range(1, nx)], base)
    base = stage(3, [(here.at(dy=k), 0) for k in range(1, ny)], base)
    sq_out[...] = sq_own[4]
    for o in range(1, nx * ny):
        remote(out_buf.at[o], in_buf.at[o], cs.at[o], cr.at[o], partner).wait_recv()
    total = acc[...]
    for o in range(1, nx * ny):
        total = total + in_buf[o].astype(jnp.float32)
    summed[...] = total.astype(jnp.bfloat16)

    def block(dz):
        return pl.ds(pl.multiple_of(here.at(dz=dz)[1] * cap, cap), cap)

    backs = []
    for j in range(1, nz):
        backs.append(
            started(
                remote(
                    summed.at[block(j), :], ret.at[block(0), :],
                    zs.at[j - 1], zr.at[j - 1], here.at(dz=j),
                )
            )
        )
    ret[block(0), :] = summed[block(0), :]
    for copy in backs:
        copy.wait_recv()
    for copy in pending:
        copy.wait_send()


def combine(sizes, part, *rest):
    ny, nz, nx, cap, width = sizes
    slots, chips = nz * cap, nx * ny
    peers = 1 + (nz - 1) + (nx - 1) + (ny - 1)
    dma = pltpu.SemaphoreType.DMA
    twice = lambda count: [dma((count,)), dma((count,))]
    vmem = pl.BlockSpec(memory_space=pltpu.VMEM)
    hid = rest[-1].shape
    slot_hid = jax.ShapeDtypeStruct((hid[0], slots), jnp.bfloat16)
    return pl.pallas_call(
        functools.partial(combine_kernel, *sizes),
        out_shape=[
            jax.ShapeDtypeStruct((slots, width), jnp.bfloat16),
            jax.ShapeDtypeStruct((8, 128), jnp.float32),
            slot_hid,
            slot_hid,
        ],
        in_specs=[vmem] * 6 + [pl.BlockSpec(memory_space=pl.ANY)],
        out_specs=[vmem] * 4,
        scratch_shapes=[
            pltpu.VMEM((hid[0], slots), jnp.float32),
            pltpu.VMEM(hid, jnp.bfloat16),
            dma(()),
            *[pltpu.VMEM((chips, slots, width), jnp.bfloat16)] * 3,
            pltpu.VMEM((slots, width), jnp.float32),
            pltpu.VMEM((slots, width), jnp.bfloat16),
            pltpu.VMEM((5, 8, 128), jnp.float32),
            pltpu.VMEM((peers, 8, 128), jnp.float32),
            *twice(chips), *twice(chips), *twice(max(1, nz - 1)), *twice(peers),
        ],
        compiler_params=pltpu.CompilerParams(
            collective_id=1, has_side_effects=True, vmem_limit_bytes=48 * 1024 * 1024
        ),
    )(part, *rest)


def on_device(sizes, count, tokens, expert_ids, route_weight, cotangent, w_gate, w_up, w_down):
    ny, experts, nx, capacity, column_width = sizes
    tok_rows, feature_width = tokens.shape
    slot_count = experts * capacity
    chosen = expert_ids[:, :, None] == jnp.arange(experts, dtype=jnp.int32)[None, None, :]
    per_token = jnp.sum(chosen.astype(jnp.bfloat16), axis=1)
    row = jnp.arange(tok_rows, dtype=jnp.int32)
    before = (row[None, :] < row[:, None]).astype(jnp.bfloat16)
    earlier = jnp.dot(before, per_token, preferred_element_type=jnp.float32).astype(jnp.int32)
    position = jnp.sum(jnp.where(chosen, earlier[:, None, :], 0), axis=2)
    slot_index = expert_ids * capacity + position
    slots = jnp.arange(slot_count, dtype=jnp.int32)
    hot = [slot_index[:, k][None, :] == slots[:, None] for k in range(2)]
    hot_any = (hot[0] | hot[1]).astype(jnp.bfloat16)
    token_slots = jnp.dot(hot_any, tokens, preferred_element_type=jnp.float32).astype(jnp.bfloat16)
    picked_cot = jnp.dot(hot_any, cotangent, preferred_element_type=jnp.float32)
    slot_weight = jnp.sum(
        jnp.where(hot[0], route_weight[:, 0][None, :], 0.0)
        + jnp.where(hot[1], route_weight[:, 1][None, :], 0.0),
        axis=1,
    )
    grad_slots = (slot_weight[:, None] * picked_cot).astype(jnp.bfloat16)
    down_weight = w_down[0]
    slot_rows, slot_grads, gate_t, up_t, hid_t, part = dispatch(
        sizes, token_slots, grad_slots, w_gate[0], w_up[0], down_weight
    )
    returned_rows, square_all, dgate_t, dup_t = combine(
        sizes, part, slot_rows, slot_grads, gate_t, up_t, hid_t, down_weight
    )
    weight_hot = [h.astype(jnp.bfloat16) for h in hot]
    picked = [against_rows(h, returned_rows) for h in weight_hot]
    layer_out = (route_weight[:, 0:1] * picked[0] + route_weight[:, 1:2] * picked[1]).astype(
        jnp.bfloat16
    )
    inv_rms = lax.rsqrt(jnp.maximum(square_all[0, 0], 0.0) / count + 1e-06)
    return (
        layer_out,
        (along(dgate_t, slot_rows) * inv_rms).astype(jnp.bfloat16)[None],
        (along(dup_t, slot_rows) * inv_rms).astype(jnp.bfloat16)[None],
        (along(hid_t, slot_grads) * inv_rms).astype(jnp.bfloat16)[None],
    )


def solution(mesh):
    ny, nz, nx = mesh.shape["dp"], mesh.shape["expert"], mesh.shape["ffn"] // CORES

    def body(*args):
        tok_rows, feature_width = args[0].shape
        sizes = (ny, nz, nx, tok_rows // 2, feature_width // (ny * nx * CORES))
        count = 3.0 * nz * args[4].shape[1] * (ny * nx * CORES) * feature_width
        return on_device(sizes, count, *args)

    return jax.shard_map(
        body,
        mesh=mesh,
        in_specs=(
            P("expert", None),
            P("expert", None),
            P("expert", None),
            P("expert", None),
            P("expert", ("dp", "ffn"), None),
            P("expert", ("dp", "ffn"), None),
            P("expert", ("dp", "ffn"), None),
        ),
        out_specs=(
            P("expert", ("dp", "ffn")),
            P("expert", ("dp", "ffn"), None),
            P("expert", ("dp", "ffn"), None),
            P("expert", ("dp", "ffn"), None),
        ),
        check_vma=False,
    )
```
